32 devices in a mesh: tm: 2 (over x), chan: 4 (over y, core), bl: 4 (over z).
Axes of the slice: x: 2, y: 2, z: 4, core: 2. Of those that a mesh axis runs over, the one named last changes fastest.
Arguments:
- voltages: bfloat16 [2, 256, 128, 512], P(None, ('chan', 'bl'), None, 'tm'), may hold values from -6 to 6
Outputs:
- visibilities: bfloat16 [2, 128, 4, 256, 256], P(None, ('chan', 'bl'), 'tm')
The draws below stay inside these ranges and needn't reach their ends.
All inputs are finite; a program needn't handle non-finite values.
Results may differ from the reference program's by a relative error of at most 0.0051.
Values may be sent and summed in bfloat16 or wider, within the bound.
A program may use at most 64 MiB of HBM per device.

```python
import jax
import jax.numpy as jnp
from jax import lax

SIG = 256
CH_DEV = 8
CHANNELS = 128
HALF = 128
TIME = 512
WIN = 4


def block_levels(stream_key, dims, pieces, least, top_value):
    gain, own = 1.0, jax.random.fold_in(stream_key, 6)
    for position, parts in pieces:
        heights = jnp.exp(jax.random.uniform(jax.random.fold_in(own, position), (parts,), jnp.float32, least / len(pieces), top_value / len(pieces)))
        gain = gain * jnp.repeat(heights, dims[position] // parts).reshape([-1 if axis == position else 1 for axis in range(len(dims))])
    return gain


def scatter_about(key, dims, deviation, limit, shards=(), kind=jnp.bfloat16):
    values = jax.random.normal(key, dims, jnp.float32) * deviation
    if len(shards) > 0:
        values = block_levels(key, dims, shards, -0.22, 0.18) * values
    return jnp.clip(values, min=-limit, max=limit).astype(kind)


def setup_inputs(seed: int = 0) -> dict:
    key_list = jax.random.split(jax.random.key(seed), 2)
    voltages = scatter_about(key_list[0], (2, SIG, CHANNELS, TIME), 1.0, 6.0, ((1, 16), (3, 2)))
    return dict(voltages=voltages)


def tapers(length):
    steps = jnp.arange(length, dtype=jnp.float32)
    taper_early = jnp.sin(jnp.pi * (steps + 0.5) / (2.0 * length))
    taper_late = jnp.sin(jnp.pi * (steps + 0.5 + length) / (2.0 * length))
    return taper_early, taper_late


def weighted(block, taper):
    return (block.astype(jnp.float32) * taper).astype(jnp.bfloat16)


def products(stacked):
    signals = stacked.shape[0] // 2
    wide = stacked.astype(jnp.float32)
    gram = jnp.einsum("pct,qct->cpq", wide, wide, precision=lax.Precision.HIGHEST)
    real_part = gram[:, :signals, :signals] + gram[:, signals:, signals:]
    imag_part = gram[:, signals:, :signals] - gram[:, :signals, signals:]
    return real_part, imag_part


def reference(voltages):
    taper_early, taper_late = tapers(HALF)
    groups = CHANNELS // CH_DEV
    halves = TIME // HALF
    scale = 1.0 / HALF

    def one_group(group):
        block = lax.dynamic_slice_in_dim(voltages, group * CH_DEV, CH_DEV, 2)
        stacked = block.reshape(2 * SIG, CH_DEV, TIME)
        previous = (jnp.zeros((CH_DEV, SIG, SIG), jnp.float32), jnp.zeros((CH_DEV, SIG, SIG), jnp.float32))
        real_list = []
        imag_list = []
        for index in range(halves):
            piece = stacked[:, :, index * HALF:(index + 1) * HALF]
            late_real, late_imag = products(weighted(piece, taper_late))
            real_list.append(((late_real + previous[0]) * scale).astype(jnp.bfloat16))
            imag_list.append(((late_imag + previous[1]) * scale).astype(jnp.bfloat16))
            previous = products(weighted(piece, taper_early))
        return jnp.stack([jnp.stack(real_list, 1), jnp.stack(imag_list, 1)], 0)

    result = lax.map(one_group, jnp.arange(groups, dtype=jnp.int32))
    return jnp.transpose(result, (1, 0, 2, 3, 4, 5)).reshape(2, CHANNELS, WIN, SIG, SIG)
```

```python
import functools

import jax
import jax.numpy as jnp
from jax import lax
from jax.experimental import pallas as pl
from jax.experimental.pallas import tpu as pltpu
from jax.sharding import PartitionSpec as P

HALF = 128
ROWS = 16
MESH = pl.DeviceIdType.MESH


def tapers(length):
    steps = jnp.arange(length, dtype=jnp.float32)
    taper_early = jnp.sin(jnp.pi * (steps + 0.5) / (2.0 * length))
    taper_late = jnp.sin(jnp.pi * (steps + 0.5 + length) / (2.0 * length))
    return (taper_early, taper_late)


def flipped(index, mask, size):
    if size & (size - 1):
        return lax.rem(index + mask, size)
    total, bit = 0, 1
    while bit < size:
        total = total + ((index // bit + mask // bit) % 2) * bit
        bit *= 2
    return total


def exchange(n_tm, n_chan, n_bl, x_ref, taper_ref, y_ref, recv, halo, send_sem, recv_sem, halo_send, halo_recv):
    n = n_chan * n_bl
    tm, chan, bl = lax.axis_index("tm"), lax.axis_index("chan"), lax.axis_index("bl")
    rank = chan * n_bl + bl
    own = x_ref.shape[1]
    chans = x_ref.shape[2] // n
    halves = x_ref.shape[3] // HALF
    group = ROWS // own
    n_groups = n // group

    def peer(step):
        there = flipped(bl, step // n_chan, n_bl)
        return flipped(chan, step % n_chan, n_chan), there

    barrier = pltpu.get_barrier_semaphore()

    def greet(step, carry):
        c, b = peer(step)
        pl.semaphore_signal(barrier, inc=1, device_id={"chan": c, "bl": b}, device_id_type=MESH)
        return carry

    lax.fori_loop(1, n, greet, 0)

    @pl.when(tm + 1 < n_tm)
    def _():
        pl.semaphore_signal(barrier, inc=1, device_id={"tm": tm + 1}, device_id_type=MESH)

    @pl.when(tm > 0)
    def _():
        pl.semaphore_signal(barrier, inc=1, device_id={"tm": tm - 1}, device_id_type=MESH)

    pl.semaphore_wait(barrier, n - 1 + jnp.minimum(tm, 1) + jnp.minimum(n_tm - 1 - tm, 1))

    def block(half, target):
        return x_ref.at[:, :, pl.ds(pl.multiple_of(target * chans, chans), chans), pl.ds(half * HALF, HALF)]

    def slot(half, source):
        return recv.at[half, :, pl.ds(source * own, own)]

    def outgoing(half, step):
        c, b = peer(step)
        return pltpu.make_async_remote_copy(
            src_ref=block(half, c * n_bl + b),
            dst_ref=slot(half, rank),
            send_sem=send_sem.at[half, step],
            recv_sem=recv_sem.at[half, rank],
            device_id={"chan": c, "bl": b},
            device_id_type=MESH,
        )

    for half in reversed(range(halves)):
        pltpu.make_async_copy(block(half, rank), slot(half, rank), recv_sem.at[half, rank]).start()

        def launch(step, carry):
            outgoing(half, step).start()
            return carry

        lax.fori_loop(1, n, launch, 0)

    def group_at(step):
        if group == 1:
            c, b = peer(step)
            return c * n_bl + b
        return lax.rem(rank // group + step, n_groups)

    def arrive(half, which):
        for member in range(group):
            source = which * group + member
            pltpu.make_async_copy(block(half, rank), slot(half, source), recv_sem.at[half, source]).wait()

    def rows(which):
        return pl.ds(pl.multiple_of(which * ROWS, ROWS), ROWS)

    def forward(which):
        return pltpu.make_async_remote_copy(
            src_ref=recv.at[halves - 1, :, rows(which)],
            dst_ref=halo.at[:, rows(which)],
            send_sem=halo_send.at[which],
            recv_sem=halo_recv.at[which],
            device_id={"tm": tm + 1},
            device_id_type=MESH,
        )

    def put(values, which, window, column, taper):
        for part in range(2):
            turned = jnp.swapaxes(values[part] * taper, 0, 1).astype(jnp.bfloat16)
            y_ref[window, :, rows(which), column + part * HALF : column + (part + 1) * HALF] = turned

    early = taper_ref[0:1, :].reshape(1, 1, HALF)
    late = taper_ref[1:2, :].reshape(1, 1, HALF)

    def last_half(step, carry):
        which = group_at(step)
        arrive(halves - 1, which)

        @pl.when(tm + 1 < n_tm)
        def _():
            forward(which).start()

        values = recv[halves - 1, :, rows(which)].astype(jnp.float32)
        put(values, which, halves - 1, 0, late)
        return carry

    lax.fori_loop(0, n_groups, last_half, 0)

    for half in range(halves - 1):

        def other_half(step, carry):
            which = group_at(step)
            arrive(half, which)
            values = recv[half, :, rows(which)].astype(jnp.float32)
            put(values, which, half, 0, late)
            put(values, which, half + 1, 2 * HALF, early)
            if half == 0:

                @pl.when(tm > 0)
                def _():
                    forward(which).wait_recv()
                    put(halo[:, rows(which)].astype(jnp.float32), which, 0, 2 * HALF, early)

                @pl.when(tm == 0)
                def _():
                    y_ref[0, :, rows(which), 2 * HALF :] = jnp.zeros((chans, ROWS, 2 * HALF), jnp.bfloat16)

            return carry

        lax.fori_loop(0, n_groups, other_half, 0)

    for half in range(halves):

        def sent(step, carry):
            outgoing(half, step).wait_send()
            return carry

        lax.fori_loop(1, n, sent, 0)

    @pl.when(tm + 1 < n_tm)
    def _():
        def passed(step, carry):
            forward(step).wait_send()
            return carry

        lax.fori_loop(0, n_groups, passed, 0)


def correlate(y_ref, out_ref):
    scale = 1.0 / HALF
    for window in range(y_ref.shape[0]):
        y = y_ref[window, 0]
        a_late, b_late = y[:, :HALF], y[:, HALF : 2 * HALF]
        a_early, b_early = y[:, 2 * HALF : 3 * HALF], y[:, 3 * HALF :]
        swapped = jnp.concatenate([b_late, -a_late, b_early, -a_early], axis=1)
        dims = (((1,), (1,)), ((), ()))
        real = lax.dot_general(y, y, dims, preferred_element_type=jnp.float32)
        imag = lax.dot_general(swapped, y, dims, preferred_element_type=jnp.float32)
        out_ref[0, 0, window] = (real * scale).astype(out_ref.dtype)
        out_ref[1, 0, window] = (imag * scale).astype(out_ref.dtype)


def solution(mesh):
    n_tm, n_chan, n_bl = (mesh.shape[axis] for axis in ("tm", "chan", "bl"))
    n = n_chan * n_bl

    def local(voltages):
        own, channels, samples = voltages.shape[1:]
        signals = own * n
        chans = channels // n
        halves = samples // HALF
        n_groups = signals // ROWS
        block = (signals, chans, HALF)
        y = pl.pallas_call(
            functools.partial(exchange, n_tm, n_chan, n_bl),
            out_shape=jax.ShapeDtypeStruct((halves, chans, signals, 4 * HALF), jnp.bfloat16),
            in_specs=[pl.BlockSpec(memory_space=pl.ANY), pl.BlockSpec(memory_space=pltpu.VMEM)],
            out_specs=pl.BlockSpec(memory_space=pltpu.VMEM),
            scratch_shapes=[
                pltpu.VMEM((halves, 2) + block, jnp.bfloat16),
                pltpu.VMEM((2,) + block, jnp.bfloat16),
                pltpu.SemaphoreType.DMA((halves, n)),
                pltpu.SemaphoreType.DMA((halves, n)),
                pltpu.SemaphoreType.DMA((n_groups,)),
                pltpu.SemaphoreType.DMA((n_groups,)),
            ],
            compiler_params=pltpu.CompilerParams(
                collective_id=0, has_side_effects=True, vmem_limit_bytes=32 * 1024 * 1024
            ),
        )(voltages, jnp.stack(tapers(HALF)))
        return pl.pallas_call(
            correlate,
            grid=(chans,),
            out_shape=jax.ShapeDtypeStruct((2, chans, halves, signals, signals), jnp.bfloat16),
            in_specs=[pl.BlockSpec((halves, 1, signals, 4 * HALF), lambda c: (0, c, 0, 0))],
            out_specs=pl.BlockSpec((2, 1, halves, signals, signals), lambda c: (0, c, 0, 0, 0)),
            compiler_params=pltpu.CompilerParams(vmem_limit_bytes=32 * 1024 * 1024),
        )(y)

    return jax.shard_map(
        local,
        mesh=mesh,
        in_specs=(P(None, ("chan", "bl"), None, "tm"),),
        out_specs=P(None, ("chan", "bl"), "tm", None, None),
        check_vma=False,
    )
```

```python
import functools

import jax
import jax.numpy as jnp
from jax import lax
from jax.experimental import pallas as pl
from jax.experimental.pallas import tpu as pltpu
from jax.sharding import PartitionSpec as P

HALF = 128
ROWS = 16
MIB = 1024 * 1024
MESH = pl.DeviceIdType.MESH


def tapers(length):
    steps = jnp.arange(length, dtype=jnp.float32)
    taper_early = jnp.sin(jnp.pi * (steps + 0.5) / (2.0 * length))
    taper_late = jnp.sin(jnp.pi * (steps + 0.5 + length) / (2.0 * length))
    return (taper_early, taper_late)


def flipped(index, mask, size):
    if size & (size - 1):
        return lax.rem(index + mask, size)
    total, bit = 0, 1
    while bit < size:
        total = total + ((index // bit + mask // bit) % 2) * bit
        bit *= 2
    return total


def exchange(n_tm, n_chan, n_bl, source_ref, taper_ref, y_ref, x_ref, recv, halo, load_sem, send_sem, recv_sem, halo_send, halo_recv):
    n = n_chan * n_bl
    tm, chan, bl = lax.axis_index("tm"), lax.axis_index("chan"), lax.axis_index("bl")
    rank = chan * n_bl + bl
    own = x_ref.shape[1]
    chans = x_ref.shape[2] // n
    halves = x_ref.shape[3] // HALF
    group = ROWS // own
    n_groups = n // group

    def peer(step):
        there = flipped(bl, step // n_chan, n_bl)
        return flipped(chan, step % n_chan, n_chan), there

    load = pltpu.make_async_copy(source_ref, x_ref, load_sem)
    load.start()
    barrier = pltpu.get_barrier_semaphore()

    def greet(step, carry):
        c, b = peer(step)
        pl.semaphore_signal(barrier, inc=1, device_id={"chan": c, "bl": b}, device_id_type=MESH)
        return carry

    lax.fori_loop(1, n, greet, 0)

    @pl.when(tm + 1 < n_tm)
    def _():
        pl.semaphore_signal(barrier, inc=1, device_id={"tm": tm + 1}, device_id_type=MESH)

    @pl.when(tm > 0)
    def _():
        pl.semaphore_signal(barrier, inc=1, device_id={"tm": tm - 1}, device_id_type=MESH)

    pl.semaphore_wait(barrier, n - 1 + jnp.minimum(tm, 1) + jnp.minimum(n_tm - 1 - tm, 1))
    load.wait()

    def block(half, target):
        return x_ref.at[:, :, pl.ds(pl.multiple_of(target * chans, chans), chans), pl.ds(half * HALF, HALF)]

    def slot(half, source):
        return recv.at[half, :, pl.ds(source * own, own)]

    def outgoing(half, step):
        c, b = peer(step)
        return pltpu.make_async_remote_copy(
            src_ref=block(half, c * n_bl + b),
            dst_ref=slot(half, rank),
            send_sem=send_sem.at[half, step],
            recv_sem=recv_sem.at[half, rank],
            device_id={"chan": c, "bl": b},
            device_id_type=MESH,
        )

    for half in reversed(range(halves)):
        pltpu.make_async_copy(block(half, rank), slot(half, rank), recv_sem.at[half, rank]).start()

        def launch(step, carry):
            outgoing(half, step).start()
            return carry

        lax.fori_loop(1, n, launch, 0)

    def group_at(step):
        if group == 1:
            c, b = peer(step)
            return c * n_bl + b
        return lax.rem(rank // group + step, n_groups)

    def arrive(half, which):
        for member in range(group):
            source = which * group + member
            pltpu.make_async_copy(block(half, rank), slot(half, source), recv_sem.at[half, source]).wait()

    def rows(which):
        return pl.ds(pl.multiple_of(which * ROWS, ROWS), ROWS)

    def forward(which):
        return pltpu.make_async_remote_copy(
            src_ref=recv.at[halves - 1, :, rows(which)],
            dst_ref=halo.at[:, rows(which)],
            send_sem=halo_send.at[which],
            recv_sem=halo_recv.at[which],
            device_id={"tm": tm + 1},
            device_id_type=MESH,
        )

    def put(values, which, window, column, taper):
        for part in range(2):
            turned = jnp.swapaxes(values[part] * taper, 0, 1).astype(jnp.bfloat16)
            y_ref[window, :, rows(which), column + part * HALF : column + (part + 1) * HALF] = turned

    early = taper_ref[0:1, :].reshape(1, 1, HALF)
    late = taper_ref[1:2, :].reshape(1, 1, HALF)

    def last_half(step, carry):
        which = group_at(step)
        arrive(halves - 1, which)

        @pl.when(tm + 1 < n_tm)
        def _():
            forward(which).start()

        values = recv[halves - 1, :, rows(which)].astype(jnp.float32)
        put(values, which, halves - 1, 0, late)
        return carry

    lax.fori_loop(0, n_groups, last_half, 0)

    for half in range(halves - 1):

        def other_half(step, carry):
            which = group_at(step)
            arrive(half, which)
            values = recv[half, :, rows(which)].astype(jnp.float32)
            put(values, which, half, 0, late)
            put(values, which, half + 1, 2 * HALF, early)
            if half == 0:

                @pl.when(tm > 0)
                def _():
                    forward(which).wait_recv()
                    put(halo[:, rows(which)].astype(jnp.float32), which, 0, 2 * HALF, early)

                @pl.when(tm == 0)
                def _():
                    y_ref[0, :, rows(which), 2 * HALF :] = jnp.zeros((chans, ROWS, 2 * HALF), jnp.bfloat16)

            return carry

        lax.fori_loop(0, n_groups, other_half, 0)

    for half in range(halves):

        def sent(step, carry):
            outgoing(half, step).wait_send()
            return carry

        lax.fori_loop(1, n, sent, 0)

    @pl.when(tm + 1 < n_tm)
    def _():
        def passed(step, carry):
            forward(step).wait_send()
            return carry

        lax.fori_loop(0, n_groups, passed, 0)


def correlate(y_ref, out_ref):
    scale = 1.0 / HALF
    signals = y_ref.shape[2]
    c = pl.program_id(0)
    for window in range(y_ref.shape[0]):
        y = y_ref[window, c]
        a_late, b_late = y[:, :HALF], y[:, HALF : 2 * HALF]
        a_early, b_early = y[:, 2 * HALF : 3 * HALF], y[:, 3 * HALF :]
        swapped = jnp.concatenate([b_late, -a_late, b_early, -a_early], axis=1)
        both = jnp.concatenate([y, swapped], axis=0)
        dims = (((1,), (1,)), ((), ()))
        gram = lax.dot_general(both, y, dims, preferred_element_type=jnp.float32) * scale
        out_ref[0, 0, window] = gram[:signals].astype(out_ref.dtype)
        out_ref[1, 0, window] = gram[signals:].astype(out_ref.dtype)


def solution(mesh):
    n_tm, n_chan, n_bl = (mesh.shape[axis] for axis in ("tm", "chan", "bl"))
    n = n_chan * n_bl

    def local(voltages):
        own, channels, samples = voltages.shape[1:]
        signals = own * n
        chans = channels // n
        halves = samples // HALF
        n_groups = signals // ROWS
        block = (signals, chans, HALF)
        y = pl.pallas_call(
            functools.partial(exchange, n_tm, n_chan, n_bl),
            out_shape=jax.ShapeDtypeStruct((halves, chans, signals, 4 * HALF), jnp.bfloat16),
            in_specs=[pl.BlockSpec(memory_space=pltpu.HBM), pl.BlockSpec(memory_space=pltpu.VMEM)],
            out_specs=pl.BlockSpec(memory_space=pltpu.VMEM),
            scratch_shapes=[
                pltpu.VMEM(voltages.shape, jnp.bfloat16),
                pltpu.VMEM((halves, 2) + block, jnp.bfloat16),
                pltpu.VMEM((2,) + block, jnp.bfloat16),
                pltpu.SemaphoreType.DMA,
                pltpu.SemaphoreType.DMA((halves, n)),
                pltpu.SemaphoreType.DMA((halves, n)),
                pltpu.SemaphoreType.DMA((n_groups,)),
                pltpu.SemaphoreType.DMA((n_groups,)),
            ],
            compiler_params=pltpu.CompilerParams(
                collective_id=0, has_side_effects=True, vmem_limit_bytes=32 * MIB
            ),
        )(pltpu.with_memory_space_constraint(voltages, pltpu.HBM), jnp.stack(tapers(HALF)))
        return pl.pallas_call(
            correlate,
            grid=(chans,),
            out_shape=jax.ShapeDtypeStruct((2, chans, halves, signals, signals), jnp.bfloat16),
            in_specs=[pl.BlockSpec(memory_space=pltpu.VMEM)],
            out_specs=pl.BlockSpec((2, 1, halves, signals, signals), lambda c: (0, c, 0, 0, 0)),
            compiler_params=pltpu.CompilerParams(vmem_limit_bytes=32 * MIB),
        )(y)

    return jax.shard_map(
        local,
        mesh=mesh,
        in_specs=(P(None, ("chan", "bl"), None, "tm"),),
        out_specs=P(None, ("chan", "bl"), "tm", None, None),
        check_vma=False,
    )
```

```python
import functools

import jax
import jax.numpy as jnp
from jax import lax
from jax.experimental import pallas as pl
from jax.experimental.pallas import tpu as pltpu
from jax.sharding import PartitionSpec as P

HALF = 128
ROWS = 16
MIB = 1024 * 1024
MESH = pl.DeviceIdType.MESH


def tapers(length):
    steps = jnp.arange(length, dtype=jnp.float32)
    taper_early = jnp.sin(jnp.pi * (steps + 0.5) / (2.0 * length))
    taper_late = jnp.sin(jnp.pi * (steps + 0.5 + length) / (2.0 * length))
    return (taper_early, taper_late)


def flipped(index, mask, size):
    if size & (size - 1):
        return lax.rem(index + mask, size)
    total, bit = 0, 1
    while bit < size:
        total = total + ((index // bit + mask // bit) % 2) * bit
        bit *= 2
    return total


def gram(y):
    swapped = jnp.concatenate([y[:, HALF:], -y[:, :HALF]], axis=1)
    dims = (((1,), (1,)), ((), ()))
    return lax.dot_general(jnp.concatenate([y, swapped], axis=0), y, dims, preferred_element_type=jnp.float32)


def exchange(n_tm, n_chan, n_bl, source_ref, taper_ref, y_ref, part_ref, x_ref, aside, recv, halo, load_sem, send_sem, recv_sem, halo_send, halo_recv):
    n = n_chan * n_bl
    tm, chan, bl = lax.axis_index("tm"), lax.axis_index("chan"), lax.axis_index("bl")
    rank = chan * n_bl + bl
    own = x_ref.shape[1]
    chans = x_ref.shape[2] // n
    halves = x_ref.shape[3] // HALF
    group = ROWS // own
    n_groups = n // group

    def peer(step):
        there = flipped(bl, step // n_chan, n_bl)
        return flipped(chan, step % n_chan, n_chan), there

    load = pltpu.make_async_copy(source_ref, x_ref, load_sem)
    load.start()
    barrier = pltpu.get_barrier_semaphore()

    def greet(step, carry):
        c, b = peer(step)
        pl.semaphore_signal(barrier, inc=1, device_id={"chan": c, "bl": b}, device_id_type=MESH)
        return carry

    lax.fori_loop(1, n, greet, 0)

    @pl.when(tm + 1 < n_tm)
    def _():
        pl.semaphore_signal(barrier, inc=1, device_id={"tm": tm + 1}, device_id_type=MESH)

    @pl.when(tm > 0)
    def _():
        pl.semaphore_signal(barrier, inc=1, device_id={"tm": tm - 1}, device_id_type=MESH)

    pl.semaphore_wait(barrier, n - 1 + jnp.minimum(tm, 1) + jnp.minimum(n_tm - 1 - tm, 1))
    load.wait()

    def block(half, target):
        return x_ref.at[:, :, pl.ds(pl.multiple_of(target * chans, chans), chans), pl.ds(half * HALF, HALF)]

    def slot(half, source):
        return recv.at[half, :, pl.ds(source * own, own)]

    def outgoing(half, step):
        c, b = peer(step)
        return pltpu.make_async_remote_copy(
            src_ref=block(half, c * n_bl + b),
            dst_ref=slot(half, rank),
            send_sem=send_sem.at[half, step],
            recv_sem=recv_sem.at[half, rank],
            device_id={"chan": c, "bl": b},
            device_id_type=MESH,
        )

    for half in range(halves):
        pltpu.make_async_copy(block(half, rank), slot(half, rank), recv_sem.at[half, rank]).start()

    for first, last in ((1, n // 2), (n // 2, n)):
        for half in reversed(range(halves)):

            def launch(step, carry):
                outgoing(half, step).start()
                return carry

            lax.fori_loop(first, last, launch, 0)

    def group_at(step):
        if group == 1:
            c, b = peer(step)
            return c * n_bl + b
        return lax.rem(rank // group + step, n_groups)

    def arrive(half, which):
        for member in range(group):
            source = which * group + member
            pltpu.make_async_copy(block(half, rank), slot(half, source), recv_sem.at[half, source]).wait()

    def rows(which):
        return pl.ds(pl.multiple_of(which * ROWS, ROWS), ROWS)

    def forward(which):
        return pltpu.make_async_remote_copy(
            src_ref=recv.at[halves - 1, :, rows(which)],
            dst_ref=halo.at[:, rows(which)],
            send_sem=halo_send.at[which],
            recv_sem=halo_recv.at[which],
            device_id={"tm": tm + 1},
            device_id_type=MESH,
        )

    def turn(values):
        return [jnp.swapaxes(values[part].astype(jnp.float32), 0, 1) for part in range(2)]

    def put(turned, where, which, column, taper):
        for part in range(2):
            tapered = (turned[part] * taper).astype(jnp.bfloat16)
            where[:, rows(which), column + part * HALF : column + (part + 1) * HALF] = tapered

    early = taper_ref[0:1, :].reshape(1, 1, HALF)
    late = taper_ref[1:2, :].reshape(1, 1, HALF)

    def last_half(step, carry):
        which = group_at(step)
        arrive(1, which)

        @pl.when(tm + 1 < n_tm)
        def _():
            forward(which).start()

        put(turn(recv[1, :, rows(which)]), aside, which, 0, late)
        return carry

    lax.fori_loop(0, n_groups, last_half, 0)

    def partial(window):
        def one(c, carry):
            part_ref[window, c] = gram(aside[c])
            return carry

        lax.fori_loop(0, chans, one, 0)

    partial(1)

    @pl.when(tm > 0)
    def _():
        def before(step, carry):
            which = group_at(step)
            forward(which).wait_recv()
            put(turn(halo[:, rows(which)]), aside, which, 0, early)
            return carry

        lax.fori_loop(0, n_groups, before, 0)
        partial(0)

    @pl.when(tm == 0)
    def _():
        part_ref[0] = jnp.zeros(part_ref.shape[1:], jnp.float32)

    def first_half(step, carry):
        which = group_at(step)
        arrive(0, which)
        turned = turn(recv[0, :, rows(which)])
        put(turned, y_ref, which, 0, late)
        put(turned, y_ref, which, 2 * HALF, early)
        return carry

    lax.fori_loop(0, n_groups, first_half, 0)

    for half in range(halves):

        def sent(step, carry):
            outgoing(half, step).wait_send()
            return carry

        lax.fori_loop(1, n, sent, 0)

    @pl.when(tm + 1 < n_tm)
    def _():
        def passed(step, carry):
            forward(step).wait_send()
            return carry

        lax.fori_loop(0, n_groups, passed, 0)


def correlate(y_ref, part_ref, out_ref):
    scale = 1.0 / HALF
    signals = y_ref.shape[1]
    c = pl.program_id(0)
    for window in range(2):
        both = gram(y_ref[c, :, 2 * window * HALF : 2 * (window + 1) * HALF])
        total = (both + part_ref[window, c]) * scale
        out_ref[0, 0, window] = total[:signals].astype(out_ref.dtype)
        out_ref[1, 0, window] = total[signals:].astype(out_ref.dtype)


def solution(mesh):
    n_tm, n_chan, n_bl = (mesh.shape[axis] for axis in ("tm", "chan", "bl"))
    n = n_chan * n_bl

    def local(voltages):
        own, channels, samples = voltages.shape[1:]
        signals = own * n
        chans = channels // n
        halves = samples // HALF
        n_groups = signals // ROWS
        block = (signals, chans, HALF)
        assert halves == 2
        y, partial = pl.pallas_call(
            functools.partial(exchange, n_tm, n_chan, n_bl),
            out_shape=(
                jax.ShapeDtypeStruct((chans, signals, 4 * HALF), jnp.bfloat16),
                jax.ShapeDtypeStruct((2, chans, 2 * signals, signals), jnp.float32),
            ),
            in_specs=[pl.BlockSpec(memory_space=pltpu.HBM), pl.BlockSpec(memory_space=pltpu.VMEM)],
            out_specs=(pl.BlockSpec(memory_space=pltpu.VMEM), pl.BlockSpec(memory_space=pltpu.VMEM)),
            scratch_shapes=[
                pltpu.VMEM(voltages.shape, jnp.bfloat16),
                pltpu.VMEM((chans, signals, 2 * HALF), jnp.bfloat16),
                pltpu.VMEM((halves, 2) + block, jnp.bfloat16),
                pltpu.VMEM((2,) + block, jnp.bfloat16),
                pltpu.SemaphoreType.DMA,
                pltpu.SemaphoreType.DMA((halves, n)),
                pltpu.SemaphoreType.DMA((halves, n)),
                pltpu.SemaphoreType.DMA((n_groups,)),
                pltpu.SemaphoreType.DMA((n_groups,)),
            ],
            compiler_params=pltpu.CompilerParams(
                collective_id=0, has_side_effects=True, vmem_limit_bytes=24 * MIB
            ),
        )(pltpu.with_memory_space_constraint(voltages, pltpu.HBM), jnp.stack(tapers(HALF)))
        return pl.pallas_call(
            correlate,
            grid=(chans,),
            out_shape=jax.ShapeDtypeStruct((2, chans, halves, signals, signals), jnp.bfloat16),
            in_specs=[pl.BlockSpec(memory_space=pltpu.VMEM), pl.BlockSpec(memory_space=pltpu.VMEM)],
            out_specs=pl.BlockSpec((2, 1, halves, signals, signals), lambda c: (0, c, 0, 0, 0)),
            compiler_params=pltpu.CompilerParams(vmem_limit_bytes=24 * MIB),
        )(y, partial)

    return jax.shard_map(
        local,
        mesh=mesh,
        in_specs=(P(None, ("chan", "bl"), None, "tm"),),
        out_specs=P(None, ("chan", "bl"), "tm", None, None),
        check_vma=False,
    )
```

```python
import functools

import jax
import jax.numpy as jnp
from jax import lax
from jax.experimental import pallas as pl
from jax.experimental.pallas import tpu as pltpu
from jax.sharding import PartitionSpec as P

HALF = 128
ROWS = 16
MIB = 1024 * 1024
MESH = pl.DeviceIdType.MESH


def tapers(length):
    steps = jnp.arange(length, dtype=jnp.float32)
    taper_early = jnp.sin(jnp.pi * (steps + 0.5) / (2.0 * length))
    taper_late = jnp.sin(jnp.pi * (steps + 0.5 + length) / (2.0 * length))
    return (taper_early, taper_late)


def flipped(index, mask, size):
    if size & (size - 1):
        return lax.rem(index + mask, size)
    total, bit = 0, 1
    while bit < size:
        total = total + ((index // bit + mask // bit) % 2) * bit
        bit *= 2
    return total


def gram(y):
    swapped = jnp.concatenate([y[:, HALF:], -y[:, :HALF]], axis=1)
    dims = (((1,), (1,)), ((), ()))
    return lax.dot_general(jnp.concatenate([y, swapped], axis=0), y, dims, preferred_element_type=jnp.float32)


def exchange(n_tm, n_chan, n_bl, source_ref, taper_ref, y_ref, part_ref, x_ref, aside, recv, halo, load_sem, send_sem, recv_sem, halo_send, halo_recv):
    n = n_chan * n_bl
    tm, chan, bl = lax.axis_index("tm"), lax.axis_index("chan"), lax.axis_index("bl")
    rank = chan * n_bl + bl
    own = x_ref.shape[1]
    chans = x_ref.shape[2] // n
    halves = x_ref.shape[3] // HALF
    group = ROWS // own
    n_groups = n // group

    def peer(step):
        there = flipped(bl, step // n_chan, n_bl)
        return flipped(chan, step % n_chan, n_chan), there

    load = pltpu.make_async_copy(source_ref, x_ref, load_sem)
    load.start()
    barrier = pltpu.get_barrier_semaphore()

    def greet(step, carry):
        c, b = peer(step)
        pl.semaphore_signal(barrier, inc=1, device_id={"chan": c, "bl": b}, device_id_type=MESH)
        return carry

    lax.fori_loop(1, n, greet, 0)

    @pl.when(tm + 1 < n_tm)
    def _():
        pl.semaphore_signal(barrier, inc=1, device_id={"tm": tm + 1}, device_id_type=MESH)

    @pl.when(tm > 0)
    def _():
        pl.semaphore_signal(barrier, inc=1, device_id={"tm": tm - 1}, device_id_type=MESH)

    pl.semaphore_wait(barrier, n - 1 + jnp.minimum(tm, 1) + jnp.minimum(n_tm - 1 - tm, 1))
    load.wait()

    def block(half, target):
        return x_ref.at[:, :, pl.ds(pl.multiple_of(target * chans, chans), chans), pl.ds(half * HALF, HALF)]

    def slot(half, source):
        return recv.at[half, :, pl.ds(source * own, own)]

    def outgoing(half, step):
        c, b = peer(step)
        return pltpu.make_async_remote_copy(
            src_ref=block(half, c * n_bl + b),
            dst_ref=slot(half, rank),
            send_sem=send_sem.at[half, step],
            recv_sem=recv_sem.at[half, rank],
            device_id={"chan": c, "bl": b},
            device_id_type=MESH,
        )

    for half in range(halves):
        pltpu.make_async_copy(block(half, rank), slot(half, rank), recv_sem.at[half, rank]).start()

    inner = jnp.minimum(jnp.minimum(bl, n_bl - 1 - bl), 1)
    for offset in (inner, 1 - inner):
        for half in reversed(range(halves)):

            def launch(index, carry):
                step = index + offset * (n // 2)

                @pl.when(step > 0)
                def _():
                    outgoing(half, step).start()

                return carry

            lax.fori_loop(0, n // 2, launch, 0)

    def group_at(step):
        if group == 1:
            c, b = peer(step)
            return c * n_bl + b
        return lax.rem(rank // group + step, n_groups)

    def arrive(half, which):
        for member in range(group):
            source = which * group + member
            pltpu.make_async_copy(block(half, rank), slot(half, source), recv_sem.at[half, source]).wait()

    def rows(which):
        return pl.ds(pl.multiple_of(which * ROWS, ROWS), ROWS)

    def forward(which):
        return pltpu.make_async_remote_copy(
            src_ref=recv.at[halves - 1, :, rows(which)],
            dst_ref=halo.at[:, rows(which)],
            send_sem=halo_send.at[which],
            recv_sem=halo_recv.at[which],
            device_id={"tm": tm + 1},
            device_id_type=MESH,
        )

    def turn(values):
        return [jnp.swapaxes(values[part].astype(jnp.float32), 0, 1) for part in range(2)]

    def put(turned, where, which, column, taper):
        for part in range(2):
            tapered = (turned[part] * taper).astype(jnp.bfloat16)
            where[:, rows(which), column + part * HALF : column + (part + 1) * HALF] = tapered

    early = taper_ref[0:1, :].reshape(1, 1, HALF)
    late = taper_ref[1:2, :].reshape(1, 1, HALF)

    def last_half(step, carry):
        which = group_at(step)
        arrive(1, which)

        @pl.when(tm + 1 < n_tm)
        def _():
            forward(which).start()

        put(turn(recv[1, :, rows(which)]), aside, which, 0, late)
        return carry

    lax.fori_loop(0, n_groups, last_half, 0)

    def partial(window):
        def one(c, carry):
            part_ref[window, c] = gram(aside[c])
            return carry

        lax.fori_loop(0, chans, one, 0)

    partial(1)

    @pl.when(tm > 0)
    def _():
        def before(step, carry):
            which = group_at(step)
            forward(which).wait_recv()
            put(turn(halo[:, rows(which)]), aside, which, 0, early)
            return carry

        lax.fori_loop(0, n_groups, before, 0)
        partial(0)

    @pl.when(tm == 0)
    def _():
        part_ref[0] = jnp.zeros(part_ref.shape[1:], jnp.float32)

    def first_half(step, carry):
        which = group_at(step)
        arrive(0, which)
        turned = turn(recv[0, :, rows(which)])
        put(turned, y_ref, which, 0, late)
        put(turned, y_ref, which, 2 * HALF, early)
        return carry

    lax.fori_loop(0, n_groups, first_half, 0)

    for half in range(halves):

        def sent(step, carry):
            outgoing(half, step).wait_send()
            return carry

        lax.fori_loop(1, n, sent, 0)

    @pl.when(tm + 1 < n_tm)
    def _():
        def passed(step, carry):
            forward(step).wait_send()
            return carry

        lax.fori_loop(0, n_groups, passed, 0)


def correlate(y_ref, part_ref, out_ref):
    scale = 1.0 / HALF
    signals = y_ref.shape[1]
    c = pl.program_id(0)
    for window in range(2):
        both = gram(y_ref[c, :, 2 * window * HALF : 2 * (window + 1) * HALF])
        total = (both + part_ref[window, c]) * scale
        out_ref[0, 0, window] = total[:signals].astype(out_ref.dtype)
        out_ref[1, 0, window] = total[signals:].astype(out_ref.dtype)


def solution(mesh):
    n_tm, n_chan, n_bl = (mesh.shape[axis] for axis in ("tm", "chan", "bl"))
    n = n_chan * n_bl

    def local(voltages):
        own, channels, samples = voltages.shape[1:]
        signals = own * n
        chans = channels // n
        halves = samples // HALF
        n_groups = signals // ROWS
        block = (signals, chans, HALF)
        assert halves == 2
        y, partial = pl.pallas_call(
            functools.partial(exchange, n_tm, n_chan, n_bl),
            out_shape=(
                jax.ShapeDtypeStruct((chans, signals, 4 * HALF), jnp.bfloat16),
                jax.ShapeDtypeStruct((2, chans, 2 * signals, signals), jnp.float32),
            ),
            in_specs=[pl.BlockSpec(memory_space=pltpu.HBM), pl.BlockSpec(memory_space=pltpu.VMEM)],
            out_specs=(pl.BlockSpec(memory_space=pltpu.VMEM), pl.BlockSpec(memory_space=pltpu.VMEM)),
            scratch_shapes=[
                pltpu.VMEM(voltages.shape, jnp.bfloat16),
                pltpu.VMEM((chans, signals, 2 * HALF), jnp.bfloat16),
                pltpu.VMEM((halves, 2) + block, jnp.bfloat16),
                pltpu.VMEM((2,) + block, jnp.bfloat16),
                pltpu.SemaphoreType.DMA,
                pltpu.SemaphoreType.DMA((halves, n)),
                pltpu.SemaphoreType.DMA((halves, n)),
                pltpu.SemaphoreType.DMA((n_groups,)),
                pltpu.SemaphoreType.DMA((n_groups,)),
            ],
            compiler_params=pltpu.CompilerParams(
                collective_id=0, has_side_effects=True, vmem_limit_bytes=24 * MIB
            ),
        )(pltpu.with_memory_space_constraint(voltages, pltpu.HBM), jnp.stack(tapers(HALF)))
        return pl.pallas_call(
            correlate,
            grid=(chans,),
            out_shape=jax.ShapeDtypeStruct((2, chans, halves, signals, signals), jnp.bfloat16),
            in_specs=[pl.BlockSpec(memory_space=pltpu.VMEM), pl.BlockSpec(memory_space=pltpu.VMEM)],
            out_specs=pl.BlockSpec((2, 1, halves, signals, signals), lambda c: (0, c, 0, 0, 0)),
            compiler_params=pltpu.CompilerParams(vmem_limit_bytes=24 * MIB),
        )(y, partial)

    return jax.shard_map(
        local,
        mesh=mesh,
        in_specs=(P(None, ("chan", "bl"), None, "tm"),),
        out_specs=P(None, ("chan", "bl"), "tm", None, None),
        check_vma=False,
    )
```
